32 devices in a mesh: grp: 4 (over z), seq: 8 (over y, x, core).
Axes of the slice: x: 2, y: 2, z: 4, core: 2. Of those that a mesh axis runs over, the one named last changes fastest.
Arguments:
- latent: bfloat16 [4, 256, 32, 256], P('grp', 'seq'), may hold values from -6 to 6
- up_key: bfloat16 [4, 128, 256], replicated, may hold values from -0.5 to 0.5
- up_value: bfloat16 [4, 128, 256], replicated, may hold values from -0.5 to 0.5
- queries: bfloat16 [8, 64, 128], replicated, may hold values from -240 to 240, as said below
- lengths: int32 [8], replicated, may hold values from 1 to 1024
- block_dest: int32 [256], replicated, may hold values from 0 to 31, as said below
Outputs:
- decode_latent: bfloat16 [32, 4, 8, 32, 256], P(('grp', 'seq'))
- attended: float32 [8, 8192], replicated
The draws below stay inside these ranges and needn't reach their ends.
Inputs may be any that keep to these rules, and one draw needn't show every extreme that they name: `block_dest`: each aligned run of 32 entries (the blocks of one seq index in the prefill layout) names every decode device exactly once. `queries`: the new token's query entries, real-valued.
All inputs are finite; a program needn't handle non-finite values.
Results may differ from the reference program's by a relative error of at most 0.001.
Values may be sent and summed in bfloat16 or wider, within the bound.
A program may use at most 64 MiB of HBM per device.

```python
import jax
import jax.numpy as jnp
from jax import lax

Q_HEADS = 64
KV_HEADS = 8
HEAD_DIM = 128
RANK = 128
BATCH = 8
BT = 32
GROUPS = 4
DESTS = 32
BLOCKS = 256
S_MAX = 1024


def draw_queries(key, part):
    drawn = jnp.clip(jax.random.normal(key, (BATCH, Q_HEADS, HEAD_DIM), jnp.float32), -4.0, 4.0)
    return drawn.astype(jnp.bfloat16)


def draw_block_dest(key, part):
    shards = BLOCKS // DESTS
    subkeys = jax.random.split(jax.random.fold_in(key, 11), shards)
    orders = jax.vmap(lambda subkey: jax.random.permutation(subkey, DESTS))(subkeys)
    return orders.reshape(BLOCKS).astype(jnp.int32)


def place_ends(values, key, least, largest):
    place = [jax.random.randint(jax.random.fold_in(key, axis), (), 0, length) for axis, length in enumerate(values.shape)]
    main_axis = values.shape.index(max(values.shape))
    next_to = place[:main_axis] + [(place[main_axis] + 1) % values.shape[main_axis]] + place[main_axis + 1:]
    return values.at[tuple(place)].set(least).at[tuple(next_to)].set(largest)


def steps_of(stream_key, shape, cuts, smallest, high):
    loudness = 1.0
    for position, blocks in cuts:
        steps = jax.random.uniform(jax.random.fold_in(jax.random.fold_in(stream_key, 6), position), (blocks,), jnp.float32, smallest / len(cuts), high / len(cuts))
        loudness = loudness * jnp.repeat(jnp.exp(steps), shape[position] // blocks).reshape((-1,) + (1,) * (len(shape) - 1 - position))
    return loudness


def noise(key, extent, spread, bound, pieces=(), kind=jnp.bfloat16):
    entries = spread * jax.random.normal(key, extent, jnp.float32)
    if pieces:
        entries = entries * steps_of(key, extent, pieces, -0.22, 0.18)
    return jnp.clip(entries, -bound, bound).astype(kind)


def setup_inputs(seed: int = 0) -> dict:
    streams_of = jax.random.split(jax.random.key(seed), 7)
    latent = noise(streams_of[0], (GROUPS, BLOCKS, BT, 2 * RANK), 1.0, 6.0, ((0, 4), (1, 8)))
    up_key = noise(streams_of[1], (GROUPS, RANK, KV_HEADS // GROUPS * HEAD_DIM), RANK ** -0.5, 0.5)
    up_value = noise(streams_of[2], (GROUPS, RANK, KV_HEADS // GROUPS * HEAD_DIM), RANK ** -0.5, 0.5)
    queries = draw_queries(jax.random.fold_in(streams_of[6], 71), 0)
    lengths = place_ends(jax.random.randint(streams_of[4], (BATCH,), 1, S_MAX + 1), jax.random.fold_in(streams_of[4], 1), 1, S_MAX).astype(jnp.int32)
    block_dest = draw_block_dest(jax.random.fold_in(streams_of[6], 71), 0)
    return dict(latent=latent, up_key=up_key, up_value=up_value, queries=queries, lengths=lengths, block_dest=block_dest)


def reference(latent, up_key, up_value, queries, lengths, block_dest):
    shards = BLOCKS // DESTS
    table = block_dest.reshape(shards, DESTS)
    row_ids = jnp.broadcast_to(jnp.arange(shards, dtype=jnp.int32)[:, None], (shards, DESTS))
    col_ids = jnp.broadcast_to(jnp.arange(DESTS, dtype=jnp.int32)[None, :], (shards, DESTS))
    source_order = jnp.zeros((shards, DESTS), jnp.int32).at[row_ids, table].set(col_ids)
    global_ids = row_ids * DESTS + source_order
    picked = latent[:, global_ids.T]
    decode_latent = jnp.transpose(picked, (1, 0, 2, 3, 4))
    per_group = KV_HEADS // GROUPS
    per_kv = Q_HEADS // KV_HEADS
    scale = 1.0 / math_sqrt(HEAD_DIM)
    query_f = queries.astype(jnp.float32).reshape(BATCH, GROUPS, per_group, per_kv, HEAD_DIM)
    positions = jnp.arange(S_MAX, dtype=jnp.int32)
    valid = positions[None, :] < lengths[:, None]

    def one_group(index):
        lat = lax.dynamic_index_in_dim(latent, index, 0, keepdims=False).astype(jnp.float32)
        lat = lat.reshape(BATCH, S_MAX, 2 * RANK)
        key_map = lax.dynamic_index_in_dim(up_key, index, 0, keepdims=False).astype(jnp.float32)
        value_map = lax.dynamic_index_in_dim(up_value, index, 0, keepdims=False).astype(jnp.float32)
        keys = jnp.einsum('bsr,rc->bsc', lat[..., :RANK], key_map, precision=lax.Precision.HIGHEST)
        values = jnp.einsum('bsr,rc->bsc', lat[..., RANK:], value_map, precision=lax.Precision.HIGHEST)
        keys = keys.reshape(BATCH, S_MAX, per_group, HEAD_DIM)
        values = values.reshape(BATCH, S_MAX, per_group, HEAD_DIM)
        query_g = lax.dynamic_index_in_dim(query_f, index, 1, keepdims=False)
        scores = jnp.einsum('bkjd,bskd->bkjs', query_g, keys, precision=lax.Precision.HIGHEST) * scale
        live = valid[:, None, None, :]
        scores = jnp.where(live, scores, -1e+30)
        row_max = lax.optimization_barrier(jnp.max(scores, axis=-1, keepdims=True))
        weights = jnp.where(live, jnp.exp(scores - row_max), 0.0)
        totals = lax.optimization_barrier(jnp.sum(weights, axis=-1))
        summed = jnp.einsum('bkjs,bskd->bkjd', weights, values, precision=lax.Precision.HIGHEST)
        return summed / totals[..., None]
    outputs = lax.map(one_group, jnp.arange(GROUPS, dtype=jnp.int32))
    attended = jnp.transpose(outputs, (1, 0, 2, 3, 4)).reshape(BATCH, Q_HEADS * HEAD_DIM)
    return (decode_latent, attended)

def math_sqrt(value):
    return float(value) ** 0.5
```

```python
import functools

import jax
import jax.numpy as jnp
from jax import lax
from jax.experimental import pallas as pl
from jax.experimental.pallas import tpu as pltpu
from jax.sharding import PartitionSpec as P

MESH = pl.DeviceIdType.MESH


def pieces(x):
    high = x.astype(jnp.bfloat16)
    rest = x - high.astype(jnp.float32)
    middle = rest.astype(jnp.bfloat16)
    low = (rest - middle.astype(jnp.float32)).astype(jnp.bfloat16)
    return jnp.concatenate([high, middle, low], axis=0)


def dot_pieces(x, y, dims):
    rows = x.shape[0]
    out = lax.dot_general(pieces(x), y, (dims, ((), ())), preferred_element_type=jnp.float32)
    return out[:rows] + (out[rows : 2 * rows] + out[2 * rows :])


def local_kernel(per_seq, per_group, per_kv, dest_ref, len_ref, lat_ref, q_ref, uk_ref, uv_ref, out_ref, part_ref):
    own_group = lax.axis_index("grp")
    own_shard = lax.axis_index("seq")
    slots, block_len, width = lat_ref.shape[1:]
    rank = width // 2
    head_dim = q_ref.shape[2]
    heads = per_group * per_kv

    @pl.loop(0, slots)
    def _(i):
        out_ref[dest_ref[own_shard * slots + i]] = lat_ref[0, i]

    sequence = own_shard // per_seq
    offset = (own_shard - sequence * per_seq) * (slots * block_len)
    left = len_ref[sequence] - offset
    tokens = slots * block_len
    query = q_ref[sequence, pl.ds(pl.multiple_of(own_group * heads, heads), heads), :]
    key_map = uk_ref[own_group]
    value_map = uv_ref[own_group]

    def cols(m, k):
        return m[:, k * head_dim : (k + 1) * head_dim]

    def rows(m, k):
        return m[k * per_kv : (k + 1) * per_kv]

    absorbed = jnp.concatenate(
        [
            rows(
                lax.dot_general(query, cols(key_map, k), (((1,), (1,)), ((), ())), preferred_element_type=jnp.float32),
                k,
            )
            for k in range(per_group)
        ],
        axis=0,
    )
    key_lat = lat_ref[0, :, :, :rank].reshape(tokens, rank)
    value_lat = lat_ref[0, :, :, rank:].reshape(tokens, rank)
    scores = dot_pieces(absorbed, key_lat, ((1,), (1,))) * (1.0 / float(head_dim) ** 0.5)
    live = lax.broadcasted_iota(jnp.int32, (heads, tokens), 1) < left
    scores = jnp.where(live, scores, -1e30)
    largest = jnp.max(scores, axis=1, keepdims=True)
    weights = jnp.where(live, jnp.exp(scores - largest), 0.0)
    total = jnp.sum(weights, axis=1, keepdims=True)
    some = jnp.where(total > 0.0, total, 1.0)
    mixed = dot_pieces(weights, value_lat, ((1,), (0,))) / some
    part_ref[0:heads, :] = jnp.concatenate(
        [rows(dot_pieces(mixed, cols(value_map, k), ((1,), (0,))), k) for k in range(per_group)], axis=0
    )
    if per_seq > 1:
        size = jnp.where(total > 0.0, largest + jnp.log(some), -1e30)
        part_ref[heads : 2 * heads, :] = jnp.broadcast_to(size, (heads, head_dim))


def comm_kernel(grps, seqs, out_ref, part_ref, recv_ref, all_ref, send_a, recv_a, send_b, recv_b):
    n = grps * seqs
    me = lax.axis_index("grp") * seqs + lax.axis_index("seq")
    barrier = pltpu.get_barrier_semaphore()

    def place(k):
        to = lax.rem(me + k, n)
        return to, (to // seqs, lax.rem(to, seqs))

    @pl.loop(1, n)
    def _(k):
        pl.semaphore_signal(barrier, inc=1, device_id=place(k)[1], device_id_type=MESH)

    pl.semaphore_wait(barrier, n - 1)

    @pl.loop(1, n)
    def _(k):
        to, there = place(k)
        pltpu.make_async_remote_copy(
            src_ref=part_ref, dst_ref=all_ref.at[me], send_sem=send_b, recv_sem=recv_b,
            device_id=there, device_id_type=MESH,
        ).start()
        pltpu.make_async_remote_copy(
            src_ref=out_ref.at[to], dst_ref=recv_ref.at[me], send_sem=send_a, recv_sem=recv_a,
            device_id=there, device_id_type=MESH,
        ).start()

    recv_ref[me] = out_ref[me]
    all_ref[me] = part_ref[...]
    most = pl.ds(0, n - 1)
    for ref, sems in ((all_ref, (send_b, recv_b)), (recv_ref, (send_a, recv_a))):
        for sem in sems:
            pltpu.make_async_copy(ref.at[most], ref.at[most], sem).wait()


def body(grps, seqs, latent, up_key, up_value, queries, lengths, block_dest):
    groups = up_key.shape[0]
    slots, block_len, width = latent.shape[1:]
    batch, q_heads, head_dim = queries.shape
    per_group = up_key.shape[2] // head_dim
    heads = q_heads // groups
    per_kv = heads // per_group
    n = grps * seqs
    blk_seq = block_dest.shape[0] // batch
    per_seq = blk_seq // slots
    assert per_seq * slots == blk_seq and n == slots and groups == grps
    part_rows = heads if per_seq == 1 else 2 * heads
    vmem = pl.BlockSpec(memory_space=pltpu.VMEM)
    smem = pl.BlockSpec(memory_space=pltpu.SMEM)
    outgoing, part = pl.pallas_call(
        functools.partial(local_kernel, per_seq, per_group, per_kv),
        out_shape=(
            jax.ShapeDtypeStruct((slots, block_len, width), latent.dtype),
            jax.ShapeDtypeStruct((part_rows, head_dim), jnp.float32),
        ),
        in_specs=[smem, smem, vmem, vmem, vmem, vmem],
        out_specs=(vmem, vmem),
        name="local_part",
    )(block_dest, lengths, latent, queries, up_key, up_value)
    received, everything = pl.pallas_call(
        functools.partial(comm_kernel, grps, seqs),
        out_shape=(
            jax.ShapeDtypeStruct((n, block_len, width), latent.dtype),
            jax.ShapeDtypeStruct((n, part_rows, head_dim), jnp.float32),
        ),
        in_specs=[vmem, vmem],
        out_specs=(vmem, vmem),
        scratch_shapes=[pltpu.SemaphoreType.DMA] * 4,
        compiler_params=pltpu.CompilerParams(collective_id=0, has_side_effects=True),
        name="exchange",
    )(outgoing, part)
    decode_latent = received.reshape(1, groups, seqs, block_len, width)
    parts = everything.reshape(groups, batch, per_seq, part_rows, head_dim)
    result = parts[:, :, 0, :heads]
    if per_seq > 1:
        sizes = parts[:, :, :, heads:]
        share = jax.nn.softmax(sizes, axis=2)
        result = jnp.sum(parts[:, :, :, :heads] * share, axis=2)
    attended = jnp.transpose(result, (1, 0, 2, 3)).reshape(batch, q_heads * head_dim)
    return (decode_latent, attended)


def solution(mesh):
    return jax.shard_map(
        functools.partial(body, mesh.shape["grp"], mesh.shape["seq"]),
        mesh=mesh,
        in_specs=(P("grp", "seq", None, None), P(), P(), P(), P(), P()),
        out_specs=(P(("grp", "seq"), None, None, None, None), P()),
        check_vma=False,
    )
```

```python
import functools

import jax
import jax.numpy as jnp
from jax import lax
from jax.experimental import pallas as pl
from jax.experimental.pallas import tpu as pltpu
from jax.sharding import PartitionSpec as P

MESH = pl.DeviceIdType.MESH


def pieces(x):
    high = x.astype(jnp.bfloat16)
    rest = x - high.astype(jnp.float32)
    middle = rest.astype(jnp.bfloat16)
    low = (rest - middle.astype(jnp.float32)).astype(jnp.bfloat16)
    return jnp.concatenate([high, middle, low], axis=0)


def dot_pieces(x, y, dims):
    rows = x.shape[0]
    out = lax.dot_general(pieces(x), y, (dims, ((), ())), preferred_element_type=jnp.float32)
    return out[:rows] + (out[rows : 2 * rows] + out[2 * rows :])


def local_kernel(per_seq, per_group, per_kv, dest_ref, len_ref, lat_ref, q_ref, uk_ref, uv_ref, out_ref, part_ref):
    own_group = lax.axis_index("grp")
    own_shard = lax.axis_index("seq")
    slots, block_len, width = lat_ref.shape[1:]
    rank = width // 2
    head_dim = q_ref.shape[2]
    heads = per_group * per_kv

    @pl.loop(0, slots)
    def _(i):
        out_ref[dest_ref[own_shard * slots + i]] = lat_ref[0, i]

    sequence = own_shard // per_seq
    offset = (own_shard - sequence * per_seq) * (slots * block_len)
    left = len_ref[sequence] - offset
    tokens = slots * block_len
    query = q_ref[sequence, pl.ds(pl.multiple_of(own_group * heads, heads), heads), :]
    key_map = uk_ref[own_group]
    value_map = uv_ref[own_group]

    def cols(m, k):
        return m[:, k * head_dim : (k + 1) * head_dim]

    def rows(m, k):
        return m[k * per_kv : (k + 1) * per_kv]

    absorbed = jnp.concatenate(
        [
            rows(
                lax.dot_general(query, cols(key_map, k), (((1,), (1,)), ((), ())), preferred_element_type=jnp.float32),
                k,
            )
            for k in range(per_group)
        ],
        axis=0,
    )
    key_lat = lat_ref[0, :, :, :rank].reshape(tokens, rank)
    value_lat = lat_ref[0, :, :, rank:].reshape(tokens, rank)
    scores = dot_pieces(absorbed, key_lat, ((1,), (1,))) * (1.0 / float(head_dim) ** 0.5)
    live = lax.broadcasted_iota(jnp.int32, (heads, tokens), 1) < left
    scores = jnp.where(live, scores, -1e30)
    largest = jnp.max(scores, axis=1, keepdims=True)
    weights = jnp.where(live, jnp.exp(scores - largest), 0.0)
    total = jnp.sum(weights, axis=1, keepdims=True)
    some = jnp.where(total > 0.0, total, 1.0)
    mixed = dot_pieces(weights, value_lat, ((1,), (0,))) / some
    part_ref[0:heads, :] = jnp.concatenate(
        [rows(dot_pieces(mixed, cols(value_map, k), ((1,), (0,))), k) for k in range(per_group)], axis=0
    )
    if per_seq > 1:
        size = jnp.where(total > 0.0, largest + jnp.log(some), -1e30)
        part_ref[heads : 2 * heads, :] = jnp.broadcast_to(size, (heads, head_dim))


def comm_kernel(grps, seqs, out_ref, part_ref, recv_ref, all_ref, send_a, recv_a, send_b, recv_b, recv_z):
    n = grps * seqs
    group = lax.axis_index("grp")
    shard = lax.axis_index("seq")
    me = group * seqs + shard
    mine = shard * grps + group
    barrier = pltpu.get_barrier_semaphore()

    def place(k):
        to = lax.rem(me + k, n)
        return to, (to // seqs, lax.rem(to, seqs))

    def send(src, dst, there, send_sem, recv_sem):
        pltpu.make_async_remote_copy(
            src_ref=src, dst_ref=dst, send_sem=send_sem, recv_sem=recv_sem, device_id=there, device_id_type=MESH
        ).start()

    @pl.loop(1, n)
    def _(k):
        pl.semaphore_signal(barrier, inc=1, device_id=place(k)[1], device_id_type=MESH)

    pl.semaphore_wait(barrier, n - 1)

    @pl.loop(1, grps)
    def _(k):
        send(part_ref, all_ref.at[mine], (lax.rem(group + k, grps), shard), send_b, recv_z)

    @pl.loop(0, n - 1)
    def _(j):
        to, there = place(1 + lax.rem(j + n // 2 - 1, n - 1))
        send(out_ref.at[to], recv_ref.at[me], there, send_a, recv_a)

    @pl.loop(1, seqs)
    def _(k):
        send(part_ref, all_ref.at[mine], (group, lax.rem(shard + k, seqs)), send_b, recv_b)

    recv_ref[me] = out_ref[me]
    all_ref[mine] = part_ref[...]

    def wait(ref, count, sem):
        some = ref.at[pl.ds(0, count)]
        pltpu.make_async_copy(some, some, sem).wait()

    wait(all_ref, grps - 1, recv_z)

    @pl.loop(1, grps)
    def _(j):
        held = all_ref.at[shard * grps + lax.rem(group + j, grps)]

        @pl.loop(1, seqs)
        def _(k):
            send(held, held, (group, lax.rem(shard + k, seqs)), send_b, recv_b)

    wait(all_ref, n - grps, recv_b)
    wait(recv_ref, n - 1, recv_a)
    wait(all_ref, n - 1, send_b)
    wait(recv_ref, n - 1, send_a)


def body(grps, seqs, latent, up_key, up_value, queries, lengths, block_dest):
    groups = up_key.shape[0]
    slots, block_len, width = latent.shape[1:]
    batch, q_heads, head_dim = queries.shape
    per_group = up_key.shape[2] // head_dim
    heads = q_heads // groups
    per_kv = heads // per_group
    n = grps * seqs
    blk_seq = block_dest.shape[0] // batch
    per_seq = blk_seq // slots
    assert per_seq * slots == blk_seq and n == slots and groups == grps
    part_rows = heads if per_seq == 1 else 2 * heads
    vmem = pl.BlockSpec(memory_space=pltpu.VMEM)
    smem = pl.BlockSpec(memory_space=pltpu.SMEM)
    outgoing, part = pl.pallas_call(
        functools.partial(local_kernel, per_seq, per_group, per_kv),
        out_shape=(
            jax.ShapeDtypeStruct((slots, block_len, width), latent.dtype),
            jax.ShapeDtypeStruct((part_rows, head_dim), jnp.float32),
        ),
        in_specs=[smem, smem, vmem, vmem, vmem, vmem],
        out_specs=(vmem, vmem),
        name="local_part",
    )(block_dest, lengths, latent, queries, up_key, up_value)
    received, everything = pl.pallas_call(
        functools.partial(comm_kernel, grps, seqs),
        out_shape=(
            jax.ShapeDtypeStruct((n, block_len, width), latent.dtype),
            jax.ShapeDtypeStruct((n, part_rows, head_dim), jnp.float32),
        ),
        in_specs=[vmem, vmem],
        out_specs=(vmem, vmem),
        scratch_shapes=[pltpu.SemaphoreType.DMA] * 5,
        compiler_params=pltpu.CompilerParams(collective_id=0, has_side_effects=True),
        name="exchange",
    )(outgoing, part)
    decode_latent = received.reshape(1, groups, seqs, block_len, width)
    parts = everything.reshape(batch, per_seq, groups, part_rows, head_dim)
    result = parts[:, 0, :, :heads]
    if per_seq > 1:
        share = jax.nn.softmax(parts[:, :, :, heads:], axis=1)
        result = jnp.sum(parts[:, :, :, :heads] * share, axis=1)
    attended = result.reshape(batch, q_heads * head_dim)
    return (decode_latent, attended)


def solution(mesh):
    return jax.shard_map(
        functools.partial(body, mesh.shape["grp"], mesh.shape["seq"]),
        mesh=mesh,
        in_specs=(P("grp", "seq", None, None), P(), P(), P(), P(), P()),
        out_specs=(P(("grp", "seq"), None, None, None, None), P()),
        check_vma=False,
    )
```

```python
import functools

import jax
import jax.numpy as jnp
from jax import lax
from jax.experimental import pallas as pl
from jax.experimental.pallas import tpu as pltpu
from jax.sharding import PartitionSpec as P

MESH = pl.DeviceIdType.MESH


def pieces(x):
    high = x.astype(jnp.bfloat16)
    rest = x - high.astype(jnp.float32)
    middle = rest.astype(jnp.bfloat16)
    low = (rest - middle.astype(jnp.float32)).astype(jnp.bfloat16)
    return jnp.concatenate([high, middle, low], axis=0)


def dot_pieces(x, y, dims):
    rows = x.shape[0]
    out = lax.dot_general(pieces(x), y, (dims, ((), ())), preferred_element_type=jnp.float32)
    return out[:rows] + (out[rows : 2 * rows] + out[2 * rows :])


def local_kernel(per_seq, per_group, per_kv, dest_ref, len_ref, lat_ref, q_ref, uk_ref, uv_ref, out_ref, part_ref):
    own_group = lax.axis_index("grp")
    own_shard = lax.axis_index("seq")
    slots, block_len, width = lat_ref.shape[1:]
    rank = width // 2
    head_dim = q_ref.shape[2]
    heads = per_group * per_kv

    @pl.loop(0, slots)
    def _(i):
        out_ref[dest_ref[own_shard * slots + i]] = lat_ref[0, i]

    sequence = own_shard // per_seq
    offset = (own_shard - sequence * per_seq) * (slots * block_len)
    left = len_ref[sequence] - offset
    tokens = slots * block_len
    query = q_ref[sequence, pl.ds(pl.multiple_of(own_group * heads, heads), heads), :]
    key_map = uk_ref[own_group]
    value_map = uv_ref[own_group]

    def cols(m, k):
        return m[:, k * head_dim : (k + 1) * head_dim]

    def rows(m, k):
        return m[k * per_kv : (k + 1) * per_kv]

    absorbed = jnp.concatenate(
        [
            rows(
                lax.dot_general(query, cols(key_map, k), (((1,), (1,)), ((), ())), preferred_element_type=jnp.float32),
                k,
            )
            for k in range(per_group)
        ],
        axis=0,
    )
    key_lat = lat_ref[0, :, :, :rank].reshape(tokens, rank)
    value_lat = lat_ref[0, :, :, rank:].reshape(tokens, rank)
    scores = dot_pieces(absorbed, key_lat, ((1,), (1,))) * (1.0 / float(head_dim) ** 0.5)
    live = lax.broadcasted_iota(jnp.int32, (heads, tokens), 1) < left
    scores = jnp.where(live, scores, -1e30)
    largest = jnp.max(scores, axis=1, keepdims=True)
    weights = jnp.where(live, jnp.exp(scores - largest), 0.0)
    total = jnp.sum(weights, axis=1, keepdims=True)
    some = jnp.where(total > 0.0, total, 1.0)
    mixed = dot_pieces(weights, value_lat, ((1,), (0,))) / some
    part_ref[0:heads, :] = jnp.concatenate(
        [rows(dot_pieces(mixed, cols(value_map, k), ((1,), (0,))), k) for k in range(per_group)], axis=0
    )
    if per_seq > 1:
        size = jnp.where(total > 0.0, largest + jnp.log(some), -1e30)
        part_ref[heads : 2 * heads, :] = jnp.broadcast_to(size, (heads, head_dim))


def comm_kernel(grps, seqs, out_ref, part_ref, recv_ref, all_ref, send_a, recv_a, send_b, recv_b, recv_z):
    n = grps * seqs
    group = lax.axis_index("grp")
    shard = lax.axis_index("seq")
    me = group * seqs + shard
    mine = shard * grps + group
    barrier = pltpu.get_barrier_semaphore()

    def place(k):
        to = lax.rem(me + k, n)
        return to, (to // seqs, lax.rem(to, seqs))

    def send(src, dst, there, send_sem, recv_sem):
        pltpu.make_async_remote_copy(
            src_ref=src, dst_ref=dst, send_sem=send_sem, recv_sem=recv_sem, device_id=there, device_id_type=MESH
        ).start()

    @pl.loop(1, n)
    def _(k):
        pl.semaphore_signal(barrier, inc=1, device_id=place(k)[1], device_id_type=MESH)

    pl.semaphore_wait(barrier, n - 1)

    @pl.loop(1, grps)
    def _(k):
        send(part_ref, all_ref.at[mine], (lax.rem(group + k, grps), shard), send_b, recv_z)

    def block(to_group, to_shard):
        send(out_ref.at[to_group * seqs + to_shard], recv_ref.at[me], (to_group, to_shard), send_a, recv_a)

    for j in range(grps - 1):
        step = 1 + (j + grps // 2 - 1) % (grps - 1)

        @pl.loop(0, seqs)
        def _(k):
            block(lax.rem(group + step, grps), lax.rem(shard + k, seqs))

    @pl.loop(1, seqs)
    def _(k):
        to_shard = lax.rem(shard + k, seqs)
        send(part_ref, all_ref.at[mine], (group, to_shard), send_b, recv_b)
        block(group, to_shard)

    recv_ref[me] = out_ref[me]
    all_ref[mine] = part_ref[...]

    def wait(ref, count, sem):
        some = ref.at[pl.ds(0, count)]
        pltpu.make_async_copy(some, some, sem).wait()

    wait(all_ref, grps - 1, recv_z)

    @pl.loop(1, grps)
    def _(j):
        held = all_ref.at[shard * grps + lax.rem(group + j, grps)]

        @pl.loop(1, seqs)
        def _(k):
            send(held, held, (group, lax.rem(shard + k, seqs)), send_b, recv_b)

    wait(all_ref, n - grps, recv_b)
    wait(recv_ref, n - 1, recv_a)
    wait(all_ref, n - 1, send_b)
    wait(recv_ref, n - 1, send_a)


def body(grps, seqs, latent, up_key, up_value, queries, lengths, block_dest):
    groups = up_key.shape[0]
    slots, block_len, width = latent.shape[1:]
    batch, q_heads, head_dim = queries.shape
    per_group = up_key.shape[2] // head_dim
    heads = q_heads // groups
    per_kv = heads // per_group
    n = grps * seqs
    blk_seq = block_dest.shape[0] // batch
    per_seq = blk_seq // slots
    assert per_seq * slots == blk_seq and n == slots and groups == grps
    part_rows = heads if per_seq == 1 else 2 * heads
    vmem = pl.BlockSpec(memory_space=pltpu.VMEM)
    smem = pl.BlockSpec(memory_space=pltpu.SMEM)
    outgoing, part = pl.pallas_call(
        functools.partial(local_kernel, per_seq, per_group, per_kv),
        out_shape=(
            jax.ShapeDtypeStruct((slots, block_len, width), latent.dtype),
            jax.ShapeDtypeStruct((part_rows, head_dim), jnp.float32),
        ),
        in_specs=[smem, smem, vmem, vmem, vmem, vmem],
        out_specs=(vmem, vmem),
        name="local_part",
    )(block_dest, lengths, latent, queries, up_key, up_value)
    received, everything = pl.pallas_call(
        functools.partial(comm_kernel, grps, seqs),
        out_shape=(
            jax.ShapeDtypeStruct((n, block_len, width), latent.dtype),
            jax.ShapeDtypeStruct((n, part_rows, head_dim), jnp.float32),
        ),
        in_specs=[vmem, vmem],
        out_specs=(vmem, vmem),
        scratch_shapes=[pltpu.SemaphoreType.DMA] * 5,
        compiler_params=pltpu.CompilerParams(collective_id=0, has_side_effects=True),
        name="exchange",
    )(outgoing, part)
    decode_latent = received.reshape(1, groups, seqs, block_len, width)
    parts = everything.reshape(batch, per_seq, groups, part_rows, head_dim)
    result = parts[:, 0, :, :heads]
    if per_seq > 1:
        share = jax.nn.softmax(parts[:, :, :, heads:], axis=1)
        result = jnp.sum(parts[:, :, :, :heads] * share, axis=1)
    attended = result.reshape(batch, q_heads * head_dim)
    return (decode_latent, attended)


def solution(mesh):
    return jax.shard_map(
        functools.partial(body, mesh.shape["grp"], mesh.shape["seq"]),
        mesh=mesh,
        in_specs=(P("grp", "seq", None, None), P(), P(), P(), P(), P()),
        out_specs=(P(("grp", "seq"), None, None, None, None), P()),
        check_vma=False,
    )
```

```python
import functools

import jax
import jax.numpy as jnp
from jax import lax
from jax.experimental import pallas as pl
from jax.experimental.pallas import tpu as pltpu
from jax.sharding import PartitionSpec as P

MESH = pl.DeviceIdType.MESH


def pieces(x):
    high = x.astype(jnp.bfloat16)
    rest = x - high.astype(jnp.float32)
    middle = rest.astype(jnp.bfloat16)
    low = (rest - middle.astype(jnp.float32)).astype(jnp.bfloat16)
    return jnp.concatenate([high, middle, low], axis=0)


def dot_pieces(x, y, dims):
    rows = x.shape[0]
    out = lax.dot_general(pieces(x), y, (dims, ((), ())), preferred_element_type=jnp.float32)
    return out[:rows] + (out[rows : 2 * rows] + out[2 * rows :])


def local_kernel(per_seq, per_group, per_kv, dest_ref, len_ref, lat_ref, q_ref, uk_ref, uv_ref, out_ref, part_ref):
    own_group = lax.axis_index("grp")
    own_shard = lax.axis_index("seq")
    slots, block_len, width = lat_ref.shape[1:]
    rank = width // 2
    head_dim = q_ref.shape[2]
    heads = per_group * per_kv

    @pl.loop(0, slots)
    def _(i):
        out_ref[dest_ref[own_shard * slots + i]] = lat_ref[0, i]

    sequence = own_shard // per_seq
    offset = (own_shard - sequence * per_seq) * (slots * block_len)
    left = len_ref[sequence] - offset
    tokens = slots * block_len
    query = q_ref[sequence, pl.ds(pl.multiple_of(own_group * heads, heads), heads), :]
    key_map = uk_ref[own_group]
    value_map = uv_ref[own_group]

    def cols(m, k):
        return m[:, k * head_dim : (k + 1) * head_dim]

    def rows(m, k):
        return m[k * per_kv : (k + 1) * per_kv]

    absorbed = jnp.concatenate(
        [
            rows(
                lax.dot_general(query, cols(key_map, k), (((1,), (1,)), ((), ())), preferred_element_type=jnp.float32),
                k,
            )
            for k in range(per_group)
        ],
        axis=0,
    )
    key_lat = lat_ref[0, :, :, :rank].reshape(tokens, rank)
    value_lat = lat_ref[0, :, :, rank:].reshape(tokens, rank)
    scores = dot_pieces(absorbed, key_lat, ((1,), (1,))) * (1.0 / float(head_dim) ** 0.5)
    live = lax.broadcasted_iota(jnp.int32, (heads, tokens), 1) < left
    scores = jnp.where(live, scores, -1e30)
    largest = jnp.max(scores, axis=1, keepdims=True)
    weights = jnp.where(live, jnp.exp(scores - largest), 0.0)
    total = jnp.sum(weights, axis=1, keepdims=True)
    some = jnp.where(total > 0.0, total, 1.0)
    mixed = dot_pieces(weights, value_lat, ((1,), (0,))) / some
    part_ref[0:heads, :] = jnp.concatenate(
        [rows(dot_pieces(mixed, cols(value_map, k), ((1,), (0,))), k) for k in range(per_group)], axis=0
    )
    if per_seq > 1:
        size = jnp.where(total > 0.0, largest + jnp.log(some), -1e30)
        part_ref[heads : 2 * heads, :] = jnp.broadcast_to(size, (heads, head_dim))


def comm_kernel(grps, seqs, per_seq, out_ref, part_ref, recv_ref, final_ref, all_ref, send_a, recv_a, send_b, recv_b, recv_z):
    n = grps * seqs
    group = lax.axis_index("grp")
    shard = lax.axis_index("seq")
    me = group * seqs + shard
    mine = shard * grps + group
    barrier = pltpu.get_barrier_semaphore()

    def place(k):
        to = lax.rem(me + k, n)
        return to, (to // seqs, lax.rem(to, seqs))

    def send(src, dst, there, send_sem, recv_sem):
        pltpu.make_async_remote_copy(
            src_ref=src, dst_ref=dst, send_sem=send_sem, recv_sem=recv_sem, device_id=there, device_id_type=MESH
        ).start()

    @pl.loop(1, n)
    def _(k):
        pl.semaphore_signal(barrier, inc=1, device_id=place(k)[1], device_id_type=MESH)

    pl.semaphore_wait(barrier, n - 1)

    @pl.loop(1, grps)
    def _(k):
        send(part_ref, all_ref.at[mine], (lax.rem(group + k, grps), shard), send_b, recv_z)

    def block(to_group, to_shard):
        send(out_ref.at[to_group * seqs + to_shard], recv_ref.at[me], (to_group, to_shard), send_a, recv_a)

    for j in range(grps - 1):
        step = 1 + (j + grps // 2 - 1) % (grps - 1)

        @pl.loop(0, seqs)
        def _(k):
            block(lax.rem(group + step, grps), lax.rem(shard + k, seqs))

    @pl.loop(1, seqs)
    def _(k):
        to_shard = lax.rem(shard + k, seqs)
        send(part_ref, all_ref.at[mine], (group, to_shard), send_b, recv_b)
        block(group, to_shard)

    recv_ref[me] = out_ref[me]
    all_ref[mine] = part_ref[...]

    def wait(ref, count, sem):
        some = ref.at[pl.ds(0, count)]
        pltpu.make_async_copy(some, some, sem).wait()

    wait(all_ref, grps - 1, recv_z)

    @pl.loop(1, grps)
    def _(j):
        held = all_ref.at[shard * grps + lax.rem(group + j, grps)]

        @pl.loop(1, seqs)
        def _(k):
            send(held, held, (group, lax.rem(shard + k, seqs)), send_b, recv_b)

    wait(all_ref, n - grps, recv_b)
    if per_seq == 1:
        heads, head_dim = part_ref.shape
        for g in range(grps):
            for h in range(heads):
                start = (g * heads + h) * head_dim
                taken = [all_ref[b * grps + g, h : h + 1, :] for b in range(seqs)]
                final_ref[:, start : start + head_dim] = jnp.concatenate(taken, axis=0)
    else:
        final_ref[...] = all_ref[...]
    wait(recv_ref, n - 1, recv_a)
    wait(all_ref, n - 1, send_b)
    wait(recv_ref, n - 1, send_a)


def body(grps, seqs, latent, up_key, up_value, queries, lengths, block_dest):
    groups = up_key.shape[0]
    slots, block_len, width = latent.shape[1:]
    batch, q_heads, head_dim = queries.shape
    per_group = up_key.shape[2] // head_dim
    heads = q_heads // groups
    per_kv = heads // per_group
    n = grps * seqs
    blk_seq = block_dest.shape[0] // batch
    per_seq = blk_seq // slots
    assert per_seq * slots == blk_seq and n == slots and groups == grps
    part_rows = heads if per_seq == 1 else 2 * heads
    final_shape = (batch, q_heads * head_dim) if per_seq == 1 else (n, part_rows, head_dim)
    vmem = pl.BlockSpec(memory_space=pltpu.VMEM)
    smem = pl.BlockSpec(memory_space=pltpu.SMEM)
    outgoing, part = pl.pallas_call(
        functools.partial(local_kernel, per_seq, per_group, per_kv),
        out_shape=(
            jax.ShapeDtypeStruct((slots, block_len, width), latent.dtype),
            jax.ShapeDtypeStruct((part_rows, head_dim), jnp.float32),
        ),
        in_specs=[smem, smem, vmem, vmem, vmem, vmem],
        out_specs=(vmem, vmem),
        name="local_part",
    )(block_dest, lengths, latent, queries, up_key, up_value)
    received, everything = pl.pallas_call(
        functools.partial(comm_kernel, grps, seqs, per_seq),
        out_shape=(
            jax.ShapeDtypeStruct((n, block_len, width), latent.dtype),
            jax.ShapeDtypeStruct(final_shape, jnp.float32),
        ),
        in_specs=[vmem, vmem],
        out_specs=(vmem, vmem),
        scratch_shapes=[pltpu.VMEM((n, part_rows, head_dim), jnp.float32)] + [pltpu.SemaphoreType.DMA] * 5,
        compiler_params=pltpu.CompilerParams(collective_id=0, has_side_effects=True),
        name="exchange",
    )(outgoing, part)
    decode_latent = received.reshape(1, groups, seqs, block_len, width)
    attended = everything
    if per_seq > 1:
        parts = everything.reshape(batch, per_seq, groups, part_rows, head_dim)
        share = jax.nn.softmax(parts[:, :, :, heads:], axis=1)
        attended = jnp.sum(parts[:, :, :, :heads] * share, axis=1).reshape(batch, q_heads * head_dim)
    return (decode_latent, attended)


def solution(mesh):
    return jax.shard_map(
        functools.partial(body, mesh.shape["grp"], mesh.shape["seq"]),
        mesh=mesh,
        in_specs=(P("grp", "seq", None, None), P(), P(), P(), P(), P()),
        out_specs=(P(("grp", "seq"), None, None, None, None), P()),
        check_vma=False,
    )
```
